32 devices in a mesh: group: 2 (over x), vocab: 16 (over z, y, core).
Axes of the slice: x: 2, y: 2, z: 4, core: 2. Of those that a mesh axis runs over, the one named last changes fastest.
Arguments:
- shard_ids: int32 [4096, 1], P(('group', 'vocab')), may hold values from 0 to 15; in each aligned block of 128 rows (0 to 127, 128 to 255, ...) at most 16 rows name the same one
- row_ids: int32 [4096], P(('group', 'vocab')), may hold values from 0 to 4007
- table: bfloat16 [64128, 4096], P('vocab', 'group'), may hold values from -6 to 6
- cotangent: bfloat16 [4096, 4096], P(('group', 'vocab')), may hold values from -6 to 6
Outputs:
- embeds: bfloat16 [4096, 4096], P(('group', 'vocab'))
- table_grad: bfloat16 [64128, 4096], P('vocab', 'group')
The draws below stay inside these ranges and needn't reach their ends.
Inputs may be any that keep to these rules, and one draw needn't show every extreme that they name: `shard_ids`: in each aligned block of 128 rows (the rows of one device), no shard is named by more than 16 rows, and in some blocks one shard is named by exactly 16.
All inputs are finite; a program needn't handle non-finite values.
Results may differ from the reference program's by a relative error of at most 0.001.
Values may be sent and summed in bfloat16 or wider, within the bound.
A program may use at most 128 MiB of HBM per device.

```python
import math
import jax
import jax.numpy as jnp
import numpy as np

D = 4096
V = 64128
TOK_DEV = 128
TOKENS = 4096
SHARD_ROWS = 4008
CAP = 16
N_VOCAB = 16


def plant(result, key, smallest, largest):
    dims = result.shape
    spot = [jax.random.randint(jax.random.fold_in(key, axis), (), 0, dims[axis]) for axis in range(len(dims))]
    result = result.at[tuple(spot)].set(smallest)
    longest = dims.index(max(dims))
    spot[longest] = (spot[longest] + 1) % dims[longest]
    return result.at[tuple(spot)].set(largest)


def block_scale(own_key, extent, shards, low, top_value):
    def one(axis_at, shards_of):
        draws = jax.random.uniform(jax.random.fold_in(jax.random.fold_in(own_key, 6), axis_at), (shards_of,), jnp.float32, low / len(shards), top_value / len(shards))
        return jnp.repeat(jnp.exp(draws), extent[axis_at] // shards_of).reshape((-1,) + (1,) * (len(extent) - axis_at - 1))

    level = one(*shards[0])
    for cut in shards[1:]:
        level = level * one(*cut)
    return level


def cumulative_ranks(amount, skew):
    loads = [(1 << 20) // math.isqrt(standing ** skew) + 1 for standing in range(1, amount + 1)]
    deviation = 1 + sum(loads) // (1 << 30)
    return np.cumsum(np.array([max(1, weight // deviation) for weight in loads]))


def ranked(stream_key, shape, number_of, slope):
    grid = cumulative_ranks(number_of, slope)
    pick = jax.random.randint(jax.random.fold_in(stream_key, 1), shape, 0, int(grid[number_of - 1]))
    grade = jnp.searchsorted(jnp.asarray(grid, jnp.int32), pick, side="right")
    return jax.random.permutation(jax.random.fold_in(stream_key, 2), number_of)[grade].astype(jnp.int32)


def shared_out(own_key, own, number, rows, amount, top, reach, skew):
    sequence = jax.random.permutation(own_key, amount)
    crowded, usual = shares(amount, rows * top, reach, skew, True), shares(amount, rows * top, reach, skew, False)
    places = jnp.arange(amount)

    def named(tallies, rotation):
        used = int((tallies > 0).sum())
        fixed = max(1, used // 4)
        moved = fixed + (places - fixed + rotation * (used - fixed)) % max(1, amount - fixed)
        return jnp.zeros((amount,), jnp.int32).at[sequence[jnp.where(places < fixed, places, moved)]].set(jnp.asarray(tallies, jnp.int32))

    tallies = jnp.where(number % 4 == 0, named(crowded, number // 4), named(usual, number - number // 4 - 1))
    mixed = jax.random.permutation(jax.random.fold_in(own, 3), amount)
    giver, sink = mixed[0:amount // 2 * 2:2], mixed[1:amount // 2 * 2:2]
    slack = jnp.minimum(tallies[giver] - 1, reach - tallies[sink]) // 2
    slack = jnp.where((giver == sequence[0]) | (sink == sequence[0]) | (tallies[sink] == 0), 0, jnp.maximum(slack, 0))
    moved = jax.random.randint(jax.random.fold_in(own, 4), (amount // 2,), 0, 1 << 20) % (slack + 1)
    tallies = tallies.at[giver].add(-moved).at[sink].add(moved)
    items = jnp.searchsorted(jnp.cumsum(tallies), jnp.arange(rows * top), side="right").astype(jnp.int32)
    listing = items.reshape(top, rows).T
    listing = listing[jax.random.permutation(jax.random.fold_in(own, 1), rows)]
    rotation = jax.random.randint(jax.random.fold_in(own, 2), (rows, 1), 0, top)
    return jnp.take_along_axis(listing, (jnp.arange(top)[None, :] + rotation) % top, axis=1)


def shares(count, total, bound, lean, full):
    weights = [(1 << 20) // math.isqrt(rank ** lean) + 1 for rank in range(1, count + 1)]
    largest = bound if full else min(bound, max(-(-total // count), total * weights[0] // sum(weights)))
    least = 1 if total - largest >= count - 1 else 0
    counts, spare = [largest] + [least] * (count - 1), total - largest - least * (count - 1)
    while spare > 0:
        free = [i for i in range(1, count) if counts[i] < largest] or [i for i in range(1, count) if counts[i] < bound]
        mass, budget = sum([weights[i] for i in free]), spare
        for i in free:
            more = min(bound - counts[i], max(1, budget * weights[i] // mass), spare)
            counts[i] = counts[i] + more
            spare = spare - more
    return np.array(counts)


def centred(stream_key, shape, spread, most, split=(), dtype=jnp.bfloat16):
    loudness = block_scale(stream_key, shape, split, -0.22, 0.18) if split else 1.0
    entries = jax.random.normal(stream_key, shape, jnp.float32) * spread * loudness
    return jnp.minimum(jnp.maximum(entries, -most), most).astype(dtype)


def setup_inputs(seed: int = 0) -> dict:
    splits = jax.random.split(jax.random.key(seed), 5)
    shard_ids_keys = jax.random.split(jax.random.fold_in(splits[0], 1), TOKENS // TOK_DEV)
    shard_ids_turns = jax.random.permutation(jax.random.fold_in(splits[0], 3), TOKENS // TOK_DEV)
    shard_ids = jax.vmap(lambda own, number: shared_out(jax.random.fold_in(splits[0], 2), own, number, TOK_DEV, N_VOCAB, 1, CAP, 2))(shard_ids_keys, shard_ids_turns).reshape((TOKENS, 1))
    row_ids = plant(ranked(splits[1], (TOKENS,), SHARD_ROWS, 2), jax.random.fold_in(splits[1], 3), 0, SHARD_ROWS - 1).astype(jnp.int32)
    table = centred(splits[2], (V, D), 1.0, 6.0, ((0, 16), (1, 2)))
    cotangent = centred(splits[3], (TOKENS, D), 1.0, 6.0, ((0, 32),))
    return {"shard_ids": shard_ids, "row_ids": row_ids, "table": table, "cotangent": cotangent}


def reference(shard_ids, row_ids, table, cotangent):
    token_ids = (shard_ids[:, 0] * (V // N_VOCAB) + row_ids).astype(jnp.int32)
    embeds = jnp.take(table, token_ids, axis=0)
    summed = jax.ops.segment_sum(cotangent.astype(jnp.float32), token_ids, num_segments=V)
    return embeds, summed.astype(jnp.bfloat16)
```

```python
import jax
import jax.numpy as jnp
from jax import lax
from jax.sharding import PartitionSpec as P

BOTH = ("group", "vocab")


def per_device(shard_ids, row_ids, table, cotangent):
    tokens, width = cotangent.shape
    groups = lax.axis_size("group")
    owners = lax.axis_size("vocab")
    per_owner = 2 * tokens // owners
    slots = owners * per_owner
    rows_here, cols = table.shape
    shard = shard_ids[:, 0]
    owner_hot = (shard[:, None] == jnp.arange(owners, dtype=jnp.int32)[None, :]).astype(jnp.bfloat16)
    earlier = jnp.tril(jnp.ones((tokens, tokens), jnp.bfloat16), -1)
    before = jnp.dot(earlier, owner_hot, preferred_element_type=jnp.float32)
    ranking = jnp.sum(before * owner_hot.astype(jnp.float32), axis=1).astype(jnp.int32)
    slot_index = shard * per_owner + ranking
    slot_hot = slot_index[:, None] == jnp.arange(slots, dtype=jnp.int32)[None, :]
    slot_mask = slot_hot.astype(jnp.bfloat16)
    outgoing = jnp.sum(jnp.where(slot_hot, (row_ids + 1)[:, None], 0), axis=0) - 1

    placed = jnp.concatenate(
        [
            lax.dot_general(
                slot_mask,
                cotangent[:, g * cols : (g + 1) * cols],
                (((0,), (0,)), ((), ())),
                preferred_element_type=jnp.float32,
            ).astype(jnp.bfloat16)
            for g in range(groups)
        ],
        axis=0,
    )
    arrived = lax.all_to_all(placed, BOTH, split_axis=0, concat_axis=0, tiled=True)

    asked = jnp.concatenate([outgoing] * groups)
    received = lax.all_to_all(asked, BOTH, split_axis=0, concat_axis=0, tiled=True)
    picker = (received[:, None] == jnp.arange(rows_here, dtype=jnp.int32)[None, :]).astype(jnp.bfloat16)
    found = jnp.dot(picker, table, preferred_element_type=jnp.float32).astype(jnp.bfloat16)
    homed = lax.all_to_all(found, BOTH, split_axis=0, concat_axis=0, tiled=True)

    table_grad = lax.dot_general(
        picker, arrived, (((0,), (0,)), ((), ())), preferred_element_type=jnp.float32
    ).astype(jnp.bfloat16)
    embeds = jnp.concatenate(
        [
            jnp.dot(
                slot_mask, homed[g * slots : (g + 1) * slots], preferred_element_type=jnp.float32
            ).astype(jnp.bfloat16)
            for g in range(groups)
        ],
        axis=1,
    )
    return embeds, table_grad


def solution(mesh):
    in_specs = (
        P(BOTH, None),
        P(BOTH),
        P("vocab", "group"),
        P(BOTH, None),
    )
    out_specs = (P(BOTH, None), P("vocab", "group"))
    return jax.shard_map(
        per_device, mesh=mesh, in_specs=in_specs, out_specs=out_specs, check_vma=False
    )
```
